256 devices in a mesh: groups: 2 (over y), ep: 16 (over z), node: 8 (over x, core).
Axes of the slice: x: 4, y: 2, z: 16, core: 2. Of those that a mesh axis runs over, the one named last changes fastest.
The devices are a block of a 4x16x16 slice.
Arguments:
- queries: bfloat16 [4096, 64, 576], P(('groups', 'ep'), 'node'), parts along dimension 0, may hold values from -16 to 16
- latent_kv: bfloat16 [4096, 576], P(('groups', 'ep')), parts along dimension 0, may hold values from -4 to 4
- w_value: bfloat16 [64, 512, 128], P('node'), may hold values from -0.25 to 0.25
- moe_tokens: bfloat16 [1024, 4096], P(('groups', 'ep')), parts along dimension 0, may hold values from -6 to 6
- routes: int32 [1024, 8], P(('groups', 'ep')), parts along dimension 0, may hold values from 0 to 15, all different within a row; in each aligned block of 32 rows (0 to 31, 32 to 63, ...) at most 24 rows name the same one
- router: bfloat16 [4096, 16], replicated, may hold values from -0.25 to 0.25
- w_gate: bfloat16 [16, 4096, 2048], P('ep', None, 'node'), may hold values from -0.09375 to 0.09375
- w_up: bfloat16 [16, 4096, 2048], P('ep', None, 'node'), may hold values from -0.09375 to 0.09375
- w_down: bfloat16 [16, 2048, 4096], P('ep', 'node'), may hold values from -0.1875 to 0.1875
Outputs:
- attention_out: bfloat16 [4096, 8192], P(('groups', 'ep'), 'node'), parts along dimension 0
- moe_out: bfloat16 [1024, 4096], P(('groups', 'ep'), 'node'), parts along dimension 0
The draws below stay inside these ranges and needn't reach their ends.
There are 2 independent parts, one for each index of `groups`. The reference program is written for one: setup_inputs(seed, part) draws one part's arguments, and reference() takes and returns one part's arrays. A program takes and returns all parts, laid end to end along the dimension named above; an argument that names none is the same for every part. Nothing has to cross between parts.
Inputs may be any that keep to these rules, and one draw needn't show every extreme that they name: `routes`: each row names 8 different experts; among the 32 rows of one index of ep no expert is named by more than 24 rows, a bound that some block reaches of them.
All inputs are finite; a program needn't handle non-finite values.
Results may differ from the reference program's by a relative error of at most 0.015.
Values may be sent and summed in bfloat16 or wider, within the bound.
A program may use at most 64 MiB of HBM per device.

```python
import math
import jax
import jax.numpy as jnp
import numpy as np
from jax import lax

D = 4096
FF = 2048
HEADS = 64
LATENT = 512
ROPE = 64
VHEAD = 128
TOPK = 8
EXPERTS = 16
SEQ_DEV = 128
SEQ = 2048
TB_DEV = 32
TOKB = 512
CAP = 24
N_EP = 16
N_NODE = 8


def attention_pair(key):
    width = LATENT + ROPE
    latent_key, query_key = jax.random.split(jax.random.fold_in(key, 11), 2)
    latent = jnp.clip(jax.random.normal(latent_key, (SEQ, width), jnp.float32), -4.0, 4.0)
    queries = jnp.clip(jax.random.normal(query_key, (SEQ, HEADS, width), jnp.float32), -4.0, 4.0)
    return (latent, queries)


def draw_queries(key, part):
    return attention_pair(key)[1].astype(jnp.bfloat16)


def draw_latent_kv(key, part):
    return attention_pair(key)[0].astype(jnp.bfloat16)


def with_spikes(entries, own_key, source, target, parts, factor):
    owner, partner = [(jnp.arange(entries.shape[position]) // (entries.shape[position] // parts)).reshape([-1 if axis == position else 1 for axis in range(entries.ndim)]) for position in (source, target)]
    chosen = jax.random.permutation(own_key, parts)[partner]
    strong = (owner == chosen) | (owner == (partner + parts // 2) % parts)
    return jnp.where(strong, factor * entries, entries)


def levels(own_key, extent, cuts, smallest, largest):
    factor_of = 1.0
    for position, blocks in cuts:
        heights = jax.random.uniform(jax.random.fold_in(jax.random.fold_in(own_key, 6), position), (blocks,), jnp.float32, smallest / len(cuts), largest / len(cuts))
        factor_of = factor_of * jnp.repeat(jnp.exp(heights), extent[position] // blocks).reshape((-1,) + (1,) * (len(extent) - 1 - position))
    return factor_of


def deal_out(key, own, number, rows, count, top, reach, skew):
    order = jax.random.permutation(key, count)
    heavy_load, usual = portions_of(count, rows * top, reach, skew, True), portions_of(count, rows * top, reach, skew, False)
    places = jnp.arange(count)

    def named(lengths, offset_by):
        used = int((lengths > 0).sum())
        fixed = max(1, used // 4)
        shifted = fixed + (places - fixed + offset_by * (used - fixed)) % max(1, count - fixed)
        return jnp.zeros((count,), jnp.int32).at[order[jnp.where(places < fixed, places, shifted)]].set(jnp.asarray(lengths, jnp.int32))

    lengths = jnp.where(number % 4 == 0, named(heavy_load, number // 4), named(usual, number - number // 4 - 1))
    mixed = jax.random.permutation(jax.random.fold_in(own, 3), count)
    giver, sink = mixed[0:count // 2 * 2:2], mixed[1:count // 2 * 2:2]
    slack = jnp.minimum(lengths[giver] - 1, reach - lengths[sink]) // 2
    slack = jnp.where((giver == order[0]) | (sink == order[0]) | (lengths[sink] == 0), 0, jnp.maximum(slack, 0))
    shifted = jax.random.randint(jax.random.fold_in(own, 4), (count // 2,), 0, 1 << 20) % (slack + 1)
    lengths = lengths.at[giver].add(-shifted).at[sink].add(shifted)
    members = jnp.searchsorted(jnp.cumsum(lengths), jnp.arange(rows * top), side="right").astype(jnp.int32)
    listing = members.reshape(top, rows).T
    listing = listing[jax.random.permutation(jax.random.fold_in(own, 1), rows)]
    offset_by = jax.random.randint(jax.random.fold_in(own, 2), (rows, 1), 0, top)
    return jnp.take_along_axis(listing, (jnp.arange(top)[None, :] + offset_by) % top, axis=1)


def portions_of(amount, total, reach, lean, full):
    loads = [(1 << 20) // math.isqrt(standing ** lean) + 1 for standing in range(1, amount + 1)]
    largest = reach if full else min(reach, max(-(-total // amount), total * loads[0] // sum(loads)))
    least = 1 if total - largest >= amount - 1 else 0
    holding, surplus = [largest] + [least] * (amount - 1), total - largest - least * (amount - 1)
    while surplus > 0:
        movable = [i for i in range(1, amount) if holding[i] < largest] or [i for i in range(1, amount) if holding[i] < reach]
        mass, budget = sum([loads[i] for i in movable]), surplus
        for i in movable:
            addition = min(reach - holding[i], max(1, budget * loads[i] // mass), surplus)
            holding[i] = holding[i] + addition
            surplus = surplus - addition
    return np.array(holding)


def gaussian(stream_key, shape, spread, most, cuts=(), kind=jnp.bfloat16):
    loudness = levels(stream_key, shape, cuts, -0.22, 0.18) if cuts else 1.0
    array = jax.random.normal(stream_key, shape, jnp.float32) * spread * loudness
    return jnp.minimum(jnp.maximum(array, -most), most).astype(kind)


def bell_draw_with(own_key, dims, scale, limit, shards, heavy, kind=jnp.bfloat16):
    values = scale * jax.random.normal(own_key, dims, jnp.float32)
    if shards:
        values = values * levels(own_key, dims, shards, -0.22, 0.18)
    return jnp.clip(with_spikes(values, jax.random.fold_in(own_key, 3), *heavy), -limit, limit).astype(kind)


def setup_inputs(seed: int = 0, part: int = 0) -> dict:
    streams_of = jax.random.split(jax.random.key(seed), 10)
    part_keys = jax.random.split(jax.random.fold_in(streams_of[9], part), 10)
    queries = draw_queries(jax.random.fold_in(jax.random.fold_in(streams_of[9], part), 71), part)
    latent_kv = draw_latent_kv(jax.random.fold_in(jax.random.fold_in(streams_of[9], part), 71), part)
    w_value = gaussian(streams_of[2], (HEADS, LATENT, VHEAD), LATENT ** -0.5, 0.25, ((0, 8),))
    moe_tokens = gaussian(part_keys[3], (TOKB, D), 1.0, 6.0, ((0, 16),))
    routes_keys = jax.random.split(jax.random.fold_in(part_keys[4], 1), TOKB // TB_DEV)
    routes_turns = jax.random.permutation(jax.random.fold_in(part_keys[4], 3), TOKB // TB_DEV)
    routes = jax.vmap(lambda own, number: deal_out(jax.random.fold_in(part_keys[4], 2), own, number, TB_DEV, EXPERTS, TOPK, CAP, 1))(routes_keys, routes_turns).reshape((TOKB, TOPK))
    router = gaussian(streams_of[5], (D, EXPERTS), (D // 9) ** -0.5, 0.25)
    w_gate = gaussian(streams_of[6], (EXPERTS, D, FF), D ** -0.5, 0.09375, ((0, 16), (2, 8)))
    w_up = gaussian(streams_of[7], (EXPERTS, D, FF), D ** -0.5, 0.09375, ((0, 16), (2, 8)))
    w_down = bell_draw_with(streams_of[8], (EXPERTS, FF, D), FF ** -0.5, 0.1875, ((0, 16), (1, 8)), (1, 2, 8, 2.0))
    return dict(queries=queries, latent_kv=latent_kv, w_value=w_value, moe_tokens=moe_tokens, routes=routes, router=router, w_gate=w_gate, w_up=w_up, w_down=w_down)


ROUTED_SCALE = 2.5


def attend_rows(block, first, latent_kv, w_value):
    width = latent_kv.shape[1]
    latent_width = w_value.shape[1]
    scale = (w_value.shape[2] + width - latent_width) ** -0.5
    scores = jnp.einsum("qhc,kc->qhk", block.astype(jnp.float32), latent_kv.astype(jnp.float32)) * scale
    query_pos = first + jnp.arange(block.shape[0], dtype=jnp.int32)
    key_pos = jnp.arange(latent_kv.shape[0], dtype=jnp.int32)
    visible = key_pos[None, None, :] <= query_pos[:, None, None]
    scores = jnp.where(visible, scores, -1.0e30)
    row_max = jnp.max(scores, axis=2, keepdims=True)
    raised = jnp.where(visible, jnp.exp(scores - row_max), 0.0)
    totals = jnp.sum(raised, axis=2, keepdims=True)
    probs = lax.optimization_barrier(raised.astype(jnp.bfloat16)).astype(jnp.float32)
    values = latent_kv[:, :latent_width].astype(jnp.float32)
    context = jnp.einsum("qhk,kc->qhc", probs, values) / totals
    context = lax.optimization_barrier(context.astype(jnp.bfloat16)).astype(jnp.float32)
    result = jnp.einsum("qhc,hcv->qhv", context, w_value.astype(jnp.float32))
    return result.astype(jnp.bfloat16).reshape(block.shape[0], -1)


def attention_part(queries, latent_kv, w_value):
    blocks = queries.reshape(N_EP, SEQ_DEV, queries.shape[1], queries.shape[2])
    firsts = jnp.arange(N_EP, dtype=jnp.int32) * SEQ_DEV

    def one_block(packed):
        return attend_rows(packed[0], packed[1], latent_kv, w_value)

    outputs = lax.map(one_block, (blocks, firsts))
    return outputs.reshape(queries.shape[0], -1)


def moe_part(moe_tokens, routes, router, w_gate, w_up, w_down):
    tokens_all, top = routes.shape
    experts = router.shape[1]
    logits = jnp.dot(moe_tokens, router, preferred_element_type=jnp.float32)
    affinity = jax.nn.sigmoid(logits)
    chosen = jnp.take_along_axis(affinity, routes, axis=1)
    gates = ROUTED_SCALE * chosen / jnp.sum(chosen, axis=1, keepdims=True)
    blocks = routes.reshape(N_EP, TB_DEV, top)
    expert_range = jnp.arange(experts, dtype=jnp.int32)
    member = jnp.any(blocks[:, :, :, None] == expert_range[None, None, None, :], axis=2).astype(jnp.int32)
    before = jnp.cumsum(member, axis=1) - member
    slots = jnp.take_along_axis(before, blocks, axis=2)
    rows = (jnp.arange(N_EP, dtype=jnp.int32)[:, None, None] * CAP + slots).reshape(-1)
    expert_ids = routes.reshape(-1)
    token_ids = jnp.repeat(jnp.arange(tokens_all, dtype=jnp.int32), top)
    table = jnp.zeros((experts, N_EP * CAP), jnp.int32).at[expert_ids, rows].set(token_ids)
    weights = jnp.zeros((experts, N_EP * CAP), jnp.float32).at[expert_ids, rows].set(gates.reshape(-1))

    def one_expert(total, packed):
        row_ids, row_gates, gate_w, up_w, down_w = packed
        inputs = moe_tokens[row_ids]
        gate = jnp.dot(inputs, gate_w, preferred_element_type=jnp.float32)
        upward = jnp.dot(inputs, up_w, preferred_element_type=jnp.float32)
        hidden = lax.optimization_barrier((jax.nn.silu(gate) * upward).astype(jnp.bfloat16)).astype(jnp.float32)
        pieces = hidden.reshape(row_ids.shape[0], N_NODE, -1)
        downs = down_w.reshape(N_NODE, -1, down_w.shape[1]).astype(jnp.float32)
        partial_value = jnp.einsum("rbf,bfd->rbd", pieces, downs)
        partial_value = lax.optimization_barrier(partial_value.astype(jnp.bfloat16)).astype(jnp.float32)
        summed = jnp.sum(partial_value, axis=1)
        return total.at[row_ids].add(row_gates[:, None] * summed), None

    start = jnp.zeros((tokens_all, moe_tokens.shape[1]), jnp.float32)
    total, ignored = lax.scan(one_expert, start, (table, weights, w_gate, w_up, w_down))
    return total.astype(jnp.bfloat16)


def reference(queries, latent_kv, w_value, moe_tokens, routes, router, w_gate, w_up, w_down):
    attention_out = attention_part(queries, latent_kv, w_value)
    moe_out = moe_part(moe_tokens, routes, router, w_gate, w_up, w_down)
    return (attention_out, moe_out)
```

```python
import functools

import jax
import jax.numpy as jnp
from jax import lax
from jax.experimental import pallas as pl
from jax.experimental.pallas import tpu as pltpu
from jax.sharding import Mesh
from jax.sharding import PartitionSpec as P

NODE = ("node_0", "node_1")
ROUTED_SCALE = 2.5
NEGATIVE = -1e30
MESH = pl.DeviceIdType.MESH
BF = jnp.bfloat16
F32 = jnp.float32
NEAR = 9


def slots_of(d):
    return (2 * d - 1, 2 * d + 1) if d < 8 else (15, 16)


def kernel(
    scale,
    tok, lat, q_hbm, wg_hbm, wu_hbm, wd_hbm, wv_hbm,
    out_a, out_m,
    X, LT, Q, WG, WU, WD, WV, S, SE, MX, CTX, HID, O, DB, XS, XR, ZS, ZR, FS, FR,
    z_s, z_r, x_s, x_r, d_s, d_r, l_s, l_r, lx_s, lx_r, ld_s, ld_r,
    rd_s, rd_r, rx_s, rx_r, rz_s, rz_r, f_s, f_r, loc,
):
    n_ep = lax.axis_size("ep")
    n_x = lax.axis_size("node_0")
    z = lax.axis_index("ep")
    c = lax.axis_index("node_0")
    k = lax.axis_index("node_1")
    p = lax.rem(c, 2)
    above = {"ep": lax.rem(z + 1, n_ep)}
    below = {"ep": lax.rem(z + n_ep - 1, n_ep)}
    right = {"node_0": lax.rem(c + 1, n_x)}
    left = {"node_0": lax.rem(c + n_x - 1, n_x)}
    across = {"node_0": lax.rem(c + 2, n_x)}
    partner = {"node_1": 1 - k}
    give = {"node_0": lax.rem(c + n_x + 1 - 2 * k, n_x)}
    send_back = {"node_0": lax.rem(c + n_x - 1 + 2 * k, n_x)}
    tile = p * 2 + k

    barrier = pltpu.get_barrier_semaphore()
    for peer in (above, below, right, left, across, partner):
        pl.semaphore_signal(barrier, inc=1, device_id=peer, device_id_type=MESH)

    local = [pltpu.make_async_copy(q_hbm, Q, loc.at[0])]
    local.append(pltpu.make_async_copy(wg_hbm.at[0], WG, loc.at[1]))
    local.append(pltpu.make_async_copy(wu_hbm.at[0], WU, loc.at[2]))
    local.append(pltpu.make_async_copy(wv_hbm, WV, loc.at[3]))
    for n in range(8):
        local.append(
            pltpu.make_async_copy(
                wd_hbm.at[0, :, n * 512 : (n + 1) * 512], WD.at[n], loc.at[4 + n]
            )
        )

    def remote(src, dst, s, r, peer):
        return pltpu.make_async_remote_copy(
            src_ref=src, dst_ref=dst, send_sem=s, recv_sem=r, device_id=peer, device_id_type=MESH
        )

    own_x = (p, p + 2)
    sent = []

    def go(copy):
        copy.start()
        sent.append(copy)

    def z_copy(d, way, h):
        dst = 2 * d - 1 + way
        src = tok.at[2 * own_x[h] + k] if d == 1 else X.at[own_x[h], k, dst - 2]
        return remote(
            src, X.at[own_x[h], k, dst], z_s.at[way, h, d - 1], z_r.at[way, h, d - 1],
            below if way else above,
        )

    def l_copy(d, way):
        dst = 2 * d - 1 + way
        src = lat.at[pl.ds(pl.multiple_of(tile * 32, 32), 32)] if d == 1 else LT.at[p, k, dst - 2]
        return remote(
            src, LT.at[p, k, dst], l_s.at[way, d - 1], l_r.at[way, d - 1], below if way else above
        )

    def x_copy(d, h):
        a, b = slots_of(d)
        ref = X.at[own_x[h], k, a:b]
        return remote(ref, ref, x_s.at[h, d - 1], x_r.at[h, d - 1], give)

    def x_wait(d, h):
        a, b = slots_of(d)
        ref = X.at[1 - p + 2 * h, k, a:b]
        remote(ref, ref, x_s.at[h, d - 1], x_r.at[h, d - 1], give).wait_recv()

    def lx_copy(d):
        a, b = slots_of(d)
        ref = LT.at[p, k, a:b]
        return remote(ref, ref, lx_s.at[d - 1], lx_r.at[d - 1], give)

    def lx_wait(d):
        a, b = slots_of(d)
        ref = LT.at[1 - p, k, a:b]
        remote(ref, ref, lx_s.at[d - 1], lx_r.at[d - 1], give).wait_recv()

    def d_copy(d, core):
        a, b = slots_of(d)
        ref = X.at[:, core, a:b]
        return remote(ref, ref, d_s.at[d - 1], d_r.at[d - 1], partner)

    def ld_copy(d, core):
        a, b = slots_of(d)
        ref = LT.at[:, core, a:b]
        return remote(ref, ref, ld_s.at[d - 1], ld_r.at[d - 1], partner)

    def ways(d):
        return (0, 1) if d < 8 else (0,)

    def keys_of(d):
        a, b = slots_of(d)
        return LT[:, :, a:b].reshape(128 * (b - a), 640)

    def scores_first():
        keys = lat[...][:, :576]

        def body(t, carry):
            rows = pl.ds(pl.multiple_of(t * 256, 256), 256)
            s = lax.dot_general(Q[rows], keys, (((1,), (1,)), ((), ())), preferred_element_type=F32)
            query = t * 32 + lax.broadcasted_iota(jnp.int32, s.shape, 0) // 8
            key = lax.broadcasted_iota(jnp.int32, s.shape, 1)
            s = jnp.where(key <= query, s, NEGATIVE)
            SE[0, rows] = s
            MX[rows] = s
            return carry

        lax.fori_loop(0, 4, body, 0)

    def scores(d):
        a, b = slots_of(d)
        keys = keys_of(d)[:, :576]
        size = 128 * (b - a)
        low = jnp.where(z >= d, 0.0, NEGATIVE).astype(F32)
        high = jnp.where(z + d >= n_ep, 0.0, NEGATIVE).astype(F32)
        if d < 8:
            at = lax.broadcasted_iota(jnp.int32, (1, size), 1)
            bias = jnp.where((at // 32) % 2 == 0, low, high)
        else:
            bias = low

        def body(t, carry):
            rows = pl.ds(pl.multiple_of(t * 256, 256), 256)
            s = lax.dot_general(Q[rows], keys, (((1,), (1,)), ((), ())), preferred_element_type=F32)
            s = s + bias
            if d < 8:
                S[d - 1, rows] = s
                MX[rows] = jnp.maximum(MX[rows], jnp.maximum(s[:, :128], s[:, 128:]))
            else:
                SE[1, rows] = s
                MX[rows] = jnp.maximum(MX[rows], s)
            return carry

        lax.fori_loop(0, 4, body, 0)

    def context(t):
        rows = pl.ds(t * 256, 256)
        top = jnp.max(MX[rows], axis=1, keepdims=True)
        s = SE[0, rows]
        e = jnp.exp((s - top) * scale)
        total = e
        acc = jnp.dot(e.astype(BF), lat[...][:, :512], preferred_element_type=F32)
        for d in range(1, 9):
            s = S[d - 1, rows] if d < 8 else SE[1, rows]
            e = jnp.exp((s - top) * scale)
            total = total + (e[:, :128] + e[:, 128:] if d < 8 else e)
            acc = acc + jnp.dot(e.astype(BF), keys_of(d)[:, :512], preferred_element_type=F32)
        acc = acc / jnp.sum(total, axis=1, keepdims=True)
        for n in range(4):
            CTX[n, rows] = acc[:, n * 128 : (n + 1) * 128]

    def values():
        for h in range(8):
            part = jnp.concatenate(
                [CTX[n, pl.ds(h, 128, stride=8), :].astype(BF) for n in range(4)], axis=1
            )
            out_a[:, h * 128 : (h + 1) * 128] = jnp.dot(
                part, WV[h], preferred_element_type=F32
            ).astype(BF)

    def expert_in(a, b):
        rows = 32 * (b - a)
        lhs = jnp.concatenate([X[n // 2, n % 2, a:b].reshape(rows, 512) for n in range(8)], axis=1)
        gate = jnp.dot(lhs, WG[...], preferred_element_type=F32)
        upward = jnp.dot(lhs, WU[...], preferred_element_type=F32)
        hidden = gate / (1.0 + jnp.exp(-gate)) * upward
        HID[a * 32 : b * 32] = hidden.astype(BF)

    def gates_of(a, b):
        parts = []
        if a == 0:
            parts.append(lat[0:32, 512:640])
            a = 1
        parts.append(LT[p, k, a:b, :, 512:640].reshape(32 * (b - a), 128))
        both = jnp.concatenate(parts, axis=0).astype(F32)
        lane = lax.broadcasted_iota(jnp.int32, both.shape, 1)
        mine = (lane == 64 + z) | (lane == 80 + z)
        return jnp.sum(jnp.where(mine, both, 0.0), axis=1, keepdims=True)

    def expert_out(a, b, core):
        g = gates_of(a, b)
        hidden = HID[a * 32 : b * 32]

        def body(x, carry):
            o = jnp.dot(hidden, WD[2 * x + core], preferred_element_type=F32) * g
            O[x, core, a:b] = o.astype(BF).reshape(b - a, 32, 512)
            return carry

        lax.fori_loop(0, 4, body, 0)

    GROUPS = ((0, NEAR), (9, 11), (11, 13), (13, 15), (15, 16))

    def rd_copy(i):
        a, b = GROUPS[i]
        return remote(O.at[:, 1 - k, a:b], DB.at[:, a:b], rd_s.at[i], rd_r.at[i], partner)

    def rx_copy(i):
        a, b = GROUPS[i]
        return remote(XS.at[:, a:b], XR.at[:, a:b], rx_s.at[i], rx_r.at[i], send_back)

    def pass_on(i):
        a, b = GROUPS[i]
        rd_copy(i).wait_recv()
        for h in range(2):
            x = 1 - p + 2 * h
            XS[h, a:b] = (O[x, k, a:b].astype(F32) + DB[x, a:b].astype(F32)).astype(BF)
        go(rx_copy(i))

    def summed(h, slot):
        x = own_x[h]
        return O[x, k, slot].astype(F32) + DB[x, slot].astype(F32) + XR[h, slot].astype(F32)

    def rz_copy(j, way, h):
        return remote(
            ZS.at[way, j - 1, h], ZR.at[way, j - 1, h],
            rz_s.at[way, h, j - 1], rz_r.at[way, h, j - 1], below if way else above,
        )

    for copy in local:
        copy.start()
    pl.semaphore_wait(barrier, 6)
    for h in range(2):
        for way in ways(1):
            go(z_copy(1, way, h))
    for way in ways(1):
        go(l_copy(1, way))
    for n in range(8):
        X[n // 2, n % 2, 0] = tok[n]
    local[0].wait()
    scores_first()

    for d in range(1, 9):
        for h in range(2):
            for way in ways(d):
                z_copy(d, way, h).wait_recv()
                if way in ways(d + 1) and d < 8:
                    go(z_copy(d + 1, way, h))
            go(x_copy(d, h))
        for way in ways(d):
            l_copy(d, way).wait_recv()
            if way in ways(d + 1) and d < 8:
                go(l_copy(d + 1, way))
        go(lx_copy(d))
        if d >= 2:
            for h in range(2):
                x_wait(d - 1, h)
            go(d_copy(d - 1, k))
            lx_wait(d - 1)
            go(ld_copy(d - 1, k))
        if d >= 3:
            d_copy(d - 2, 1 - k).wait_recv()
            ld_copy(d - 2, 1 - k).wait_recv()
            scores(d - 2)
        if d == 6:
            for copy in local[1:3]:
                copy.wait()
            expert_in(0, NEAR)
        if d == 7:
            for copy in local[3:]:
                copy.wait()
            expert_out(0, NEAR, 1 - k)
            go(rd_copy(0))
            expert_out(0, NEAR, k)
    for h in range(2):
        x_wait(8, h)
    go(d_copy(8, k))
    lx_wait(8)
    go(ld_copy(8, k))
    for d in (7, 8):
        d_copy(d, 1 - k).wait_recv()
        ld_copy(d, 1 - k).wait_recv()

    expert_in(NEAR, 16)
    expert_out(NEAR, 16, 1 - k)
    for i in (4, 3, 2, 1):
        go(rd_copy(i))
    expert_out(NEAR, 16, k)
    for i in (4, 3, 2, 1, 0):
        pass_on(i)

    ready = set()
    for j in range(1, 9):
        for way in (0, 1):
            if way and j == 8:
                continue
            dist = 8 - j if way else 9 - j
            slot = 2 * dist - 1 if (way or dist == 8) else 2 * dist
            i = [n for n, (a, b) in enumerate(GROUPS) if a <= slot < b][0]
            if i not in ready:
                rx_copy(i).wait_recv()
                ready.add(i)
            for h in range(2):
                total = summed(h, slot)
                if j > 1:
                    rz_copy(j - 1, way, h).wait_recv()
                    total = total + ZR[way, j - 2, h].astype(F32)
                ZS[way, j - 1, h] = total.astype(BF)
                go(rz_copy(j, way, h))
        if j == 1:
            scores(7)
        if j == 2:
            scores(8)
        if 3 <= j <= 6:
            context(j - 3)
        if j == 7:
            values()

    mine = lax.div(c, 2)
    kept = []
    for h in range(2):
        rz_copy(8, 0, h).wait_recv()
        rz_copy(7, 1, h).wait_recv()
        kept.append(summed(h, 0) + ZR[0, 7, h].astype(F32) + ZR[1, 6, h].astype(F32))
    FS[...] = jnp.where(mine == 0, kept[1], kept[0]).astype(BF)
    last = remote(FS, FR, f_s.at[0], f_r.at[0], across)
    go(last)
    last.wait_recv()
    out_m[...] = (jnp.where(mine == 0, kept[0], kept[1]) + FR[...].astype(F32)).astype(BF)
    for copy in sent:
        copy.wait_send()


def per_device(queries, latent_kv, w_value, moe_tokens, routes, router, w_gate, w_up, w_down):
    seq_dev, heads_dev, width = queries.shape
    latent_width, value_width = w_value.shape[1:]
    tokens_dev, model_width = moe_tokens.shape
    experts = router.shape[1]
    scale = (value_width + width - latent_width) ** (-0.5)

    affinity = jax.nn.sigmoid(jnp.dot(moe_tokens, router, preferred_element_type=F32))
    expert_range = lax.iota(jnp.int32, experts)
    member = jnp.any(routes[:, :, None] == expert_range[None, None, :], axis=1)
    chosen = jnp.where(member, affinity, 0.0)
    gates = ROUTED_SCALE * chosen / jnp.sum(chosen, axis=1, keepdims=True)
    high = gates.astype(BF)
    low = (gates - high.astype(F32)).astype(BF)
    extra = jnp.concatenate([high, low, jnp.zeros((tokens_dev, 32), BF)], axis=1)
    lat = jnp.concatenate([latent_kv, jnp.tile(extra, (seq_dev // tokens_dev, 1))], axis=1)

    tok = moe_tokens.reshape(tokens_dev, 8, 512).transpose(1, 0, 2)
    rows = seq_dev * heads_dev
    dma = pltpu.SemaphoreType.DMA
    vmem = pl.BlockSpec(memory_space=pltpu.VMEM)
    hbm = pl.BlockSpec(memory_space=pl.ANY)
    return pl.pallas_call(
        functools.partial(kernel, scale),
        out_shape=(
            jax.ShapeDtypeStruct((seq_dev, heads_dev * value_width), BF),
            jax.ShapeDtypeStruct((tokens_dev, 512), BF),
        ),
        in_specs=[vmem, vmem] + [hbm] * 5,
        out_specs=(vmem, vmem),
        scratch_shapes=[
            pltpu.VMEM((4, 2, 16, 32, 512), BF),
            pltpu.VMEM((2, 2, 16, 32, 640), BF),
            pltpu.VMEM((rows, width), BF),
            pltpu.VMEM((model_width, 256), BF),
            pltpu.VMEM((model_width, 256), BF),
            pltpu.VMEM((8, 256, 512), BF),
            pltpu.VMEM((heads_dev, latent_width, value_width), BF),
            pltpu.VMEM((7, rows, 256), F32),
            pltpu.VMEM((2, rows, 128), F32),
            pltpu.VMEM((rows, 128), F32),
            pltpu.VMEM((4, rows, 128), F32),
            pltpu.VMEM((512, 256), BF),
            pltpu.VMEM((4, 2, 16, 32, 512), BF),
            pltpu.VMEM((4, 16, 32, 512), BF),
            pltpu.VMEM((2, 16, 32, 512), BF),
            pltpu.VMEM((2, 16, 32, 512), BF),
            pltpu.VMEM((2, 8, 2, 32, 512), BF),
            pltpu.VMEM((2, 8, 2, 32, 512), BF),
            pltpu.VMEM((32, 512), BF),
            pltpu.VMEM((32, 512), BF),
            dma((2, 2, 8)), dma((2, 2, 8)),
            dma((2, 8)), dma((2, 8)),
            dma((8,)), dma((8,)),
            dma((2, 8)), dma((2, 8)),
            dma((8,)), dma((8,)),
            dma((8,)), dma((8,)),
            dma((5,)), dma((5,)),
            dma((5,)), dma((5,)),
            dma((2, 2, 8)), dma((2, 2, 8)),
            dma((1,)), dma((1,)),
            dma((12,)),
        ],
        compiler_params=pltpu.CompilerParams(
            collective_id=0, has_side_effects=True, vmem_limit_bytes=60 * 1024 * 1024
        ),
    )(tok, lat, queries.reshape(rows, width), w_gate, w_up, w_down, w_value)


def solution(mesh):
    torus = Mesh(
        mesh.devices.reshape(mesh.shape["groups"], mesh.shape["ep"], mesh.shape["node"] // 2, 2),
        ("groups", "ep", "node_0", "node_1"),
    )
    placed = (
        P(("groups", "ep"), NODE, None),
        P(("groups", "ep"), None),
        P(NODE, None, None),
        P(("groups", "ep"), None),
        P(("groups", "ep"), None),
        P(),
        P("ep", None, NODE),
        P("ep", None, NODE),
        P("ep", NODE, None),
    )
    return jax.shard_map(
        per_device,
        mesh=torus,
        in_specs=placed,
        out_specs=(P(("groups", "ep"), NODE), P(("groups", "ep"), NODE)),
        check_vma=False,
    )
```
